32 devices in a mesh: ta: 4 (over y, x), sa: 8 (over z, core).
Axes of the slice: x: 2, y: 2, z: 4, core: 2. Of those that a mesh axis runs over, the one named last changes fastest.
Arguments:
- eigvecs: float32 [2, 8, 64, 3, 4096], P(None, 'ta', None, None, 'sa'), may hold values from -0.0546875 to 0.0546875
- solutions: float32 [2, 8, 3, 8, 4, 3, 4096], P(None, 'ta', None, None, None, None, 'sa'), may hold values from -15 to 15
- source_times: int32 [3], replicated, may hold values from 0 to 7, as said below
- spin_dilution: int32 [3, 8], replicated, may hold values from 0 to 3
Outputs:
- perambulator: float32 [2, 8, 6144], P(None, 'ta', 'sa')
- norms: float32 [3, 8], replicated
The draws below stay inside these ranges and needn't reach their ends.
Inputs may be any that keep to these rules, and one draw needn't show every extreme that they name: `source_times`: some source lies at slice 0 and another at slice 8 - 1.
All inputs are finite; a program needn't handle non-finite values.
Results may differ from the reference program's by a relative error of at most 0.000084.
Values sent between devices are 32-bit elements; how exact they have to be, the bound alone decides.
A program may use at most 64 MiB of HBM per device.

```python
import jax
import jax.numpy as jnp
from jax import lax

NEV = 64
NSRC = 3
COLS = 8
NT = 8
NSPACE = 4096


def times_for(key):
    base = jax.random.randint(jax.random.fold_in(key, 7), (NSRC,), 0, NT).astype(jnp.int32)
    last_pick = jax.random.randint(jax.random.fold_in(key, 8), (), 0, NSRC).astype(jnp.int32)
    step_pick = jax.random.randint(jax.random.fold_in(key, 9), (), 1, NSRC).astype(jnp.int32)
    first_pick = (last_pick + step_pick) % NSRC
    slots = jnp.arange(NSRC, dtype=jnp.int32)
    base = jnp.where(slots == last_pick, NT - 1, base)
    base = jnp.where(slots == first_pick, 0, base)
    return base.astype(jnp.int32)


def draw_source_times(key, part):
    return times_for(key)


def solution_part(key, salt):
    starts = times_for(key)
    slice_ids = jnp.arange(NT, dtype=jnp.int32)
    apart = jnp.abs(slice_ids[:, None] - starts[None, :])
    apart = jnp.minimum(apart, NT - apart).astype(jnp.float32)
    amplitude = 0.5 + 2.5 * jnp.exp(-apart * 16.0 / NT)
    shape = (NT, NSRC, COLS, 4, 3, NSPACE)
    noise_key = jax.random.fold_in(key, salt)
    noise = jnp.clip(jax.random.normal(noise_key, shape, jnp.float32), -5.0, 5.0)
    return noise * amplitude[:, :, None, None, None, None]


def draw_solutions(key, part):
    return jnp.stack([solution_part(key, 11), solution_part(key, 13)]).astype(jnp.float32)


def plant(entries, key, least, high):
    longest = entries.shape.index(max(entries.shape))
    spots = []
    for shift in (0, 1):
        where = [jax.random.randint(jax.random.fold_in(key, axis), (), 0, length) for axis, length in enumerate(entries.shape)]
        where[longest] = (where[longest] + shift) % entries.shape[longest]
        spots.append(tuple(where))
    return entries.at[spots[0]].set(least).at[spots[1]].set(high)


def level_of(stream_key, extent, shards, smallest, top_value):
    level = 1.0
    for dim, shards_of in shards:
        steps = jax.random.uniform(jax.random.fold_in(jax.random.fold_in(stream_key, 6), dim), (shards_of,), jnp.float32, smallest / len(shards), top_value / len(shards))
        level = level * jnp.repeat(jnp.exp(steps), extent[dim] // shards_of).reshape((-1,) + (1,) * (len(extent) - 1 - dim))
    return level


def centred(own_key, shape, width, bound, pieces=(), held_as=jnp.bfloat16):
    loudness = level_of(own_key, shape, pieces, -0.22, 0.18) if pieces else 1.0
    array = jax.random.normal(own_key, shape, jnp.float32) * width * loudness
    return jnp.minimum(jnp.maximum(array, -bound), bound).astype(held_as)


def setup_inputs(seed: int = 0) -> dict:
    seeds = jax.random.split(jax.random.key(seed), 5)
    eigvecs = centred(seeds[0], (2, NT, NEV, 3, NSPACE), (3 * NSPACE) ** -0.5, 0.0546875, ((1, 4), (4, 8)), jnp.float32)
    solutions = draw_solutions(jax.random.fold_in(seeds[4], 71), 0)
    source_times = draw_source_times(jax.random.fold_in(seeds[4], 71), 0)
    spin_dilution = plant(jax.random.randint(seeds[3], (NSRC, COLS), 0, 4), jax.random.fold_in(seeds[3], 1), 0, 3).astype(jnp.int32)
    return dict(eigvecs=eigvecs, solutions=solutions, source_times=source_times, spin_dilution=spin_dilution)


def slice_tile(inputs):
    eig_real, eig_imag, sol_real, sol_imag = inputs
    precise = lax.Precision.HIGHEST
    real_part = jnp.dot(eig_real, sol_real.T, precision=precise, preferred_element_type=jnp.float32) + jnp.dot(eig_imag, sol_imag.T, precision=precise, preferred_element_type=jnp.float32)
    imag_part = jnp.dot(eig_real, sol_imag.T, precision=precise, preferred_element_type=jnp.float32) - jnp.dot(eig_imag, sol_real.T, precision=precise, preferred_element_type=jnp.float32)
    return jnp.stack([real_part, imag_part])


def reference(eigvecs, solutions, source_times, spin_dilution):
    slice_count = eigvecs.shape[1]
    eig_count = eigvecs.shape[2]
    site_count = eigvecs.shape[4]
    src_count = spin_dilution.shape[0]
    col_count = spin_dilution.shape[1]
    columns = src_count * col_count * 4
    inner_len = 3 * site_count
    eigen_rows = eigvecs.reshape(2, slice_count, eig_count, inner_len)
    solution_rows = solutions.reshape(2, slice_count, columns, inner_len)
    tiles = lax.map(slice_tile, (eigen_rows[0], eigen_rows[1], solution_rows[0], solution_rows[1]))
    tiles = jnp.transpose(tiles, (1, 0, 2, 3))
    slice_times = jnp.arange(slice_count, dtype=jnp.int32)
    boundary = jnp.where(slice_times[:, None] < source_times[None, :], -1.0, 1.0).astype(jnp.float32)
    chirality = jnp.where(spin_dilution < 2, 1.0, -1.0).astype(jnp.float32)
    signs = jnp.broadcast_to((boundary[:, :, None] * chirality[None])[:, :, :, None], (slice_count, src_count, col_count, 4)).reshape(slice_count, columns)
    perambulator = (tiles * signs[None, :, None, :]).reshape(2, slice_count, eig_count * columns)
    norms = jnp.sum(solutions * solutions, axis=(0, 1, 4, 5, 6)) / (12.0 * slice_count * site_count)
    return perambulator, norms
```

```python
import functools
import math

import jax
import jax.numpy as jnp
from jax import lax
from jax.experimental import pallas as pl
from jax.experimental.pallas import tpu as pltpu
from jax.sharding import PartitionSpec as P

LANES = 128
NT_DIMS = (((1,), (1,)), ((), ()))


def split_two(x):
    high = x.astype(jnp.bfloat16)
    low = (x - high.astype(jnp.float32)).astype(jnp.bfloat16)
    return high, low


def kernel(
    dims,
    eig_hbm, sol_hbm, times_ref, spin_ref,
    out_ref, norm_ref,
    eig_buf, sol_buf, left, right_hi, right_lo, tile_buf, flat_buf,
    send_buf, recv_buf, norm_send, norm_recv,
    eig_sem, sol_sem, out_sems, in_sems, norm_out_sems, norm_in_sems,
):
    n_ta, n_sa, parts, slices, eigs, colors, sites, srcs, cols, spins, width = dims
    columns = srcs * cols * spins
    rows_own = width // LANES
    blocks = sites // LANES
    my_ta, my_sa = lax.axis_index("ta"), lax.axis_index("sa")

    barrier = pltpu.get_barrier_semaphore()
    for off in range(1, n_sa):
        pl.semaphore_signal(barrier, inc=1, device_id={"sa": lax.rem(my_sa + off, n_sa)})
    for off in range(1, n_ta):
        pl.semaphore_signal(barrier, inc=1, device_id={"ta": lax.rem(my_ta + off, n_ta)})

    sol_copies, eig_copies = {}, {}
    for t in range(slices):
        for c in range(colors):
            for j in range(blocks):
                at = (t * colors + c) * blocks + j
                copy = pltpu.make_async_copy(
                    sol_hbm.at[:, t, :, c, :, pl.ds(j * LANES, LANES)],
                    sol_buf.at[at].reshape(parts, srcs * cols, spins, LANES),
                    sol_sem.at[at],
                )
                copy.start()
                sol_copies[t, c, j] = copy
            copy = pltpu.make_async_copy(
                eig_hbm.at[:, t, c], eig_buf.at[t * colors + c], eig_sem.at[t * colors + c]
            )
            copy.start()
            eig_copies[t, c] = copy

    lane = lax.broadcasted_iota(jnp.int32, (8, LANES), 1)
    chir = jnp.ones((8, LANES), jnp.float32)
    group = lane // spins
    for s in range(srcs):
        for k in range(cols):
            value = jnp.where(spin_ref[s, k] < 2, 1.0, -1.0)
            chir = jnp.where(group == s * cols + k, value, chir)
    source = lane // (spins * cols)
    signs = []
    for t in range(slices):
        now = my_ta * slices + t
        sign = chir
        for s in range(srcs):
            value = jnp.where(now < times_ref[s], -1.0, 1.0)
            sign = jnp.where(source == s, chir * value, sign)
        signs.append(sign[:1])

    inner = colors * sites
    pad = LANES - columns
    if pad:
        for t in range(slices):
            for p in range(parts):
                rows = pl.ds(p * LANES + columns, pad)
                right_hi[t, rows, :] = jnp.zeros((pad, inner), jnp.bfloat16)
                right_lo[t, rows, :] = jnp.zeros((pad, inner), jnp.bfloat16)
    squares = jnp.zeros((columns, LANES), jnp.float32)
    for t in range(slices):
        for c in range(colors):
            for j in range(blocks):
                sol_copies[t, c, j].wait()
                lanes = pl.ds(c * sites + j * LANES, LANES)
                for p in range(parts):
                    x = sol_buf[(t * colors + c) * blocks + j, p]
                    squares = squares + x * x
                    high, low = split_two(x)
                    right_hi[t, pl.ds(p * LANES, columns), lanes] = high
                    right_lo[t, pl.ds(p * LANES, columns), lanes] = low
            eig_copies[t, c].wait()
            lanes = pl.ds(c * sites, sites)
            for p in range(parts):
                high, low = split_two(eig_buf[t * colors + c, p])
                left[t, pl.ds(p * eigs, eigs), lanes] = high
                left[t, pl.ds((parts + p) * eigs, eigs), lanes] = low

    pl.semaphore_wait(barrier, n_sa + n_ta - 2)

    precise = lax.Precision.HIGHEST
    lane_sums = lax.dot_general(
        jnp.ones((8, LANES), jnp.float32), squares, NT_DIMS,
        precision=precise, preferred_element_type=jnp.float32,
    )
    wanted = lax.broadcasted_iota(jnp.int32, (8, columns), 0)
    given = lax.broadcasted_iota(jnp.int32, (8, columns), 1)
    lane_sums = jnp.where(given // (spins * cols) == wanted, lane_sums, 0.0)
    col_of = lax.broadcasted_iota(jnp.int32, (LANES, columns), 0)
    col_in = lax.rem(lax.broadcasted_iota(jnp.int32, (LANES, columns), 1) // spins, cols)
    picks = jnp.where(col_of == col_in, 1.0, 0.0).astype(jnp.float32)
    norm_send[...] = lax.dot_general(
        lane_sums, picks, NT_DIMS, precision=precise, preferred_element_type=jnp.float32
    )
    norm_copies = []
    for off in range(1, n_ta):
        copy = pltpu.make_async_remote_copy(
            src_ref=norm_send,
            dst_ref=norm_recv.at[off - 1],
            send_sem=norm_out_sems.at[off - 1],
            recv_sem=norm_in_sems.at[off - 1],
            device_id={"ta": lax.rem(my_ta + off, n_ta)},
        )
        copy.start()
        norm_copies.append(copy)

    period = math.lcm(columns, LANES)
    rows_in, rows_out = period // columns, period // LANES
    groups = eigs // rows_in
    lane_g = lax.broadcasted_iota(jnp.int32, (groups, LANES), 1)
    copies = {}
    for t in range(slices):
        both = lax.dot_general(
            left[t], right_hi[t], NT_DIMS, preferred_element_type=jnp.float32
        )
        cross = lax.dot_general(
            left[t, : parts * eigs, :], right_lo[t], NT_DIMS,
            preferred_element_type=jnp.float32,
        )
        g = both[: parts * eigs] + both[parts * eigs :] + cross
        tiles = (
            g[:eigs, :LANES] + g[eigs:, LANES:],
            g[:eigs, LANES:] - g[eigs:, :LANES],
        )
        for p in range(parts):
            tile_buf[t, p] = tiles[p] * signs[t]
            rows = [tile_buf[t, p, pl.ds(i, groups, stride=rows_in), :] for i in range(rows_in)]
            for o in range(rows_out):
                value, filled = None, 0
                while filled < LANES:
                    i, skip = divmod(o * LANES + filled, columns)
                    size = min(columns - skip, LANES - filled)
                    shift = (filled - skip) % LANES
                    piece = pltpu.roll(rows[i], shift, 1) if shift else rows[i]
                    value = piece if value is None else jnp.where(lane_g < filled, value, piece)
                    filled += size
                flat_buf[t, p, pl.ds(o, groups, stride=rows_out), :] = value
            for d in range(n_sa):
                send_buf[t, d, pl.ds(p * rows_own, rows_own), :] = flat_buf[
                    t, p, pl.ds(d * rows_own, rows_own), :
                ]
        if t == slices - 1:
            norm = norm_send[...]
            for off in range(1, n_ta):
                norm_copies[off - 1].wait_recv()
                norm = norm + norm_recv[off - 1]
            for d in range(n_sa):
                send_buf[t, d, pl.ds(parts * rows_own, srcs), :] = norm[:srcs]
        for off in range(1, n_sa):
            peer = lax.rem(my_sa + off, n_sa)
            copy = pltpu.make_async_remote_copy(
                src_ref=send_buf.at[t, peer],
                dst_ref=recv_buf.at[t, off - 1],
                send_sem=out_sems.at[t, off - 1],
                recv_sem=in_sems.at[t, off - 1],
                device_id={"sa": peer},
            )
            copy.start()
            copies[t, off] = copy

    for t in range(slices):
        total = send_buf[t, my_sa]
        for off in range(1, n_sa):
            copies[t, off].wait_recv()
            total = total + recv_buf[t, off - 1]
        for p in range(parts):
            for r in range(rows_own):
                row = p * rows_own + r
                out_ref[p, pl.ds(t, 1), pl.ds(r * LANES, LANES)] = total[row : row + 1]
        if t == slices - 1:
            cells = 1.0 * spins * colors * slices * n_ta * sites * n_sa
            at = parts * rows_own
            norm_ref[...] = total[at : at + srcs, :cols] / cells
    for copy in norm_copies:
        copy.wait_send()
    for copy in copies.values():
        copy.wait_send()


def on_device(eigvecs, solutions, source_times, spin_dilution):
    n_ta, n_sa = lax.axis_size("ta"), lax.axis_size("sa")
    parts, slices, eigs, colors, sites = eigvecs.shape
    _, _, srcs, cols, spins, _, _ = solutions.shape
    columns = srcs * cols * spins
    width = eigs * columns // n_sa
    eig_view = jnp.transpose(eigvecs, (0, 1, 3, 2, 4))
    sol_view = jnp.transpose(solutions, (0, 1, 2, 3, 5, 4, 6)).reshape(
        parts, slices, srcs * cols, colors, spins, sites
    )
    dims = (n_ta, n_sa, parts, slices, eigs, colors, sites, srcs, cols, spins, width)
    blocks = sites // LANES
    inner = colors * sites
    rows = -(-(parts * (width // LANES) + srcs) // 8) * 8
    f32, bf16 = jnp.float32, jnp.bfloat16
    dma = pltpu.SemaphoreType.DMA
    return pl.pallas_call(
        functools.partial(kernel, dims),
        out_shape=(
            jax.ShapeDtypeStruct((parts, slices, width), f32),
            jax.ShapeDtypeStruct((srcs, cols), f32),
        ),
        in_specs=[
            pl.BlockSpec(memory_space=pltpu.HBM),
            pl.BlockSpec(memory_space=pltpu.HBM),
            pl.BlockSpec(memory_space=pltpu.SMEM),
            pl.BlockSpec(memory_space=pltpu.SMEM),
        ],
        out_specs=(
            pl.BlockSpec(memory_space=pltpu.VMEM),
            pl.BlockSpec(memory_space=pltpu.VMEM),
        ),
        scratch_shapes=[
            pltpu.VMEM((slices * colors, parts, eigs, sites), f32),
            pltpu.VMEM((slices * colors * blocks, parts, columns, LANES), f32),
            pltpu.VMEM((slices, 2 * parts * eigs, inner), bf16),
            pltpu.VMEM((slices, parts * LANES, inner), bf16),
            pltpu.VMEM((slices, parts * LANES, inner), bf16),
            pltpu.VMEM((slices, parts, eigs, LANES), f32),
            pltpu.VMEM((slices, parts, eigs * columns // LANES, LANES), f32),
            pltpu.VMEM((slices, n_sa, rows, LANES), f32),
            pltpu.VMEM((slices, n_sa - 1, rows, LANES), f32),
            pltpu.VMEM((8, LANES), f32),
            pltpu.VMEM((n_ta - 1, 8, LANES), f32),
            dma((slices * colors,)),
            dma((slices * colors * blocks,)),
            dma((slices, n_sa - 1)),
            dma((slices, n_sa - 1)),
            dma((n_ta - 1,)),
            dma((n_ta - 1,)),
        ],
        compiler_params=pltpu.CompilerParams(collective_id=0, has_side_effects=True),
    )(eig_view, sol_view, source_times, spin_dilution)


def solution(mesh):
    return jax.shard_map(
        on_device,
        mesh=mesh,
        in_specs=(
            P(None, "ta", None, None, "sa"),
            P(None, "ta", None, None, None, None, "sa"),
            P(),
            P(),
        ),
        out_specs=(P(None, "ta", "sa"), P()),
        check_vma=False,
    )
```

```python
import functools
import math

import jax
import jax.numpy as jnp
from jax import lax
from jax.experimental import pallas as pl
from jax.experimental.pallas import tpu as pltpu
from jax.sharding import PartitionSpec as P

LANES = 128
NT_DIMS = (((1,), (1,)), ((), ()))


def split_two(x):
    high = x.astype(jnp.bfloat16)
    low = (x - high.astype(jnp.float32)).astype(jnp.bfloat16)
    return high, low


def kernel(
    dims,
    eig_hbm, sol_hbm, times_hbm, spin_hbm,
    out_ref, norm_ref,
    eig_buf, sol_buf, left, right_hi, right_lo, tile_buf, flat_buf,
    send_buf, recv_buf, norm_sa_send, norm_sa_recv, norm_ta_send, norm_ta_recv,
    times_ref, spin_ref, small_sem, own_sem,
    eig_sem, sol_sem, out_sems, in_sems, sa_out_sems, sa_in_sems, ta_out_sems, ta_in_sems,
):
    n_ta, n_sa, parts, slices, eigs, colors, sites, srcs, cols, spins, width = dims
    columns = srcs * cols * spins
    rows_own = width // LANES
    blocks = sites // LANES
    my_ta, my_sa = lax.axis_index("ta"), lax.axis_index("sa")

    barrier = pltpu.get_barrier_semaphore()
    for off in range(1, n_sa):
        pl.semaphore_signal(barrier, inc=1, device_id={"sa": lax.rem(my_sa + off, n_sa)})
    for off in range(1, n_ta):
        pl.semaphore_signal(barrier, inc=1, device_id={"ta": lax.rem(my_ta + off, n_ta)})

    small_copies = [
        pltpu.make_async_copy(times_hbm, times_ref, small_sem.at[0]),
        pltpu.make_async_copy(spin_hbm, spin_ref, small_sem.at[1]),
    ]
    for copy in small_copies:
        copy.start()
    sol_copies, eig_copies = {}, {}
    for t in range(slices):
        for c in range(colors):
            for j in range(blocks):
                at = (t * colors + c) * blocks + j
                copy = pltpu.make_async_copy(
                    sol_hbm.at[:, t, :, c, :, pl.ds(j * LANES, LANES)],
                    sol_buf.at[at].reshape(parts, srcs * cols, spins, LANES),
                    sol_sem.at[at],
                )
                copy.start()
                sol_copies[t, c, j] = copy
            copy = pltpu.make_async_copy(
                eig_hbm.at[:, t, c], eig_buf.at[t * colors + c], eig_sem.at[t * colors + c]
            )
            copy.start()
            eig_copies[t, c] = copy

    inner = colors * sites
    pad = LANES - columns
    if pad:
        for t in range(slices):
            for p in range(parts):
                rows = pl.ds(p * LANES + columns, pad)
                right_hi[t, rows, :] = jnp.zeros((pad, inner), jnp.bfloat16)
                right_lo[t, rows, :] = jnp.zeros((pad, inner), jnp.bfloat16)
    squares = jnp.zeros((columns, LANES), jnp.float32)
    for t in range(slices):
        for c in range(colors):
            for j in range(blocks):
                sol_copies[t, c, j].wait()
                lanes = pl.ds(c * sites + j * LANES, LANES)
                for p in range(parts):
                    x = sol_buf[(t * colors + c) * blocks + j, p]
                    squares = squares + x * x
                    high, low = split_two(x)
                    right_hi[t, pl.ds(p * LANES, columns), lanes] = high
                    right_lo[t, pl.ds(p * LANES, columns), lanes] = low
            eig_copies[t, c].wait()
            lanes = pl.ds(c * sites, sites)
            for p in range(parts):
                high, low = split_two(eig_buf[t * colors + c, p])
                left[t, pl.ds(p * eigs, eigs), lanes] = high
                left[t, pl.ds((parts + p) * eigs, eigs), lanes] = low

    pl.semaphore_wait(barrier, n_sa + n_ta - 2)

    precise = lax.Precision.HIGHEST
    lane_sums = lax.dot_general(
        jnp.ones((8, LANES), jnp.float32), squares, NT_DIMS,
        precision=precise, preferred_element_type=jnp.float32,
    )
    wanted = lax.broadcasted_iota(jnp.int32, (LANES, columns), 0)
    given = lax.broadcasted_iota(jnp.int32, (LANES, columns), 1) // spins
    picks = jnp.where(wanted == given, 1.0, 0.0).astype(jnp.float32)
    own_norm = lax.dot_general(
        lane_sums, picks, NT_DIMS, precision=precise, preferred_element_type=jnp.float32
    )[:1]
    norm_sa_send[...] = own_norm
    norm_sa_copies, norm_ta_copies = [], []
    for off in range(1, n_sa):
        copy = pltpu.make_async_remote_copy(
            src_ref=norm_sa_send,
            dst_ref=norm_sa_recv.at[off - 1],
            send_sem=sa_out_sems.at[off - 1],
            recv_sem=sa_in_sems.at[off - 1],
            device_id={"sa": lax.rem(my_sa + off, n_sa)},
        )
        copy.start()
        norm_sa_copies.append(copy)

    for copy in small_copies:
        copy.wait()
    lane = lax.broadcasted_iota(jnp.int32, (8, LANES), 1)
    chir = jnp.ones((8, LANES), jnp.float32)
    group = lane // spins
    for s in range(srcs):
        for k in range(cols):
            value = jnp.where(spin_ref[s, k] < 2, 1.0, -1.0)
            chir = jnp.where(group == s * cols + k, value, chir)
    source = lane // (spins * cols)
    signs = []
    for t in range(slices):
        now = my_ta * slices + t
        sign = chir
        for s in range(srcs):
            value = jnp.where(now < times_ref[s], -1.0, 1.0)
            sign = jnp.where(source == s, chir * value, sign)
        signs.append(sign[:1])

    period = math.lcm(columns, LANES)
    rows_in, rows_out = period // columns, period // LANES
    groups = eigs // rows_in
    lane_g = lax.broadcasted_iota(jnp.int32, (groups, LANES), 1)
    copies, owns = {}, []
    rows = parts * rows_own
    sub = math.gcd(rows, 4)
    for t in range(slices):
        both = lax.dot_general(
            left[t], right_hi[t], NT_DIMS, preferred_element_type=jnp.float32
        )
        cross = lax.dot_general(
            left[t, : parts * eigs, :], right_lo[t], NT_DIMS,
            preferred_element_type=jnp.float32,
        )
        g = both[: parts * eigs] + both[parts * eigs :] + cross
        tiles = (
            g[:eigs, :LANES] + g[eigs:, LANES:],
            g[:eigs, LANES:] - g[eigs:, :LANES],
        )
        for p in range(parts):
            tile_buf[t, p] = tiles[p] * signs[t]
            taken = [tile_buf[t, p, pl.ds(i, groups, stride=rows_in), :] for i in range(rows_in)]
            for o in range(rows_out):
                value, filled = None, 0
                while filled < LANES:
                    i, skip = divmod(o * LANES + filled, columns)
                    size = min(columns - skip, LANES - filled)
                    shift = (filled - skip) % LANES
                    piece = pltpu.roll(taken[i], shift, 1) if shift else taken[i]
                    value = piece if value is None else jnp.where(lane_g < filled, value, piece)
                    filled += size
                flat_buf[t, p, pl.ds(o, groups, stride=rows_out), :] = value
            for d in range(n_sa):
                send_buf[t, pl.ds(d * rows + p * rows_own, rows_own), :] = flat_buf[
                    t, p, pl.ds(d * rows_own, rows_own), :
                ]
        sent = send_buf.at[t].reshape(n_sa, rows // sub, sub, LANES)
        landed = recv_buf.at[t].reshape(n_sa, rows // sub, sub, LANES)
        for off in range(1, n_sa):
            peer = lax.rem(my_sa + off, n_sa)
            copy = pltpu.make_async_remote_copy(
                src_ref=sent.at[peer],
                dst_ref=landed.at[off - 1],
                send_sem=out_sems.at[t, off - 1],
                recv_sem=in_sems.at[t, off - 1],
                device_id={"sa": peer},
            )
            copy.start()
            copies[t, off] = copy
        own = pltpu.make_async_copy(sent.at[my_sa], landed.at[n_sa - 1], own_sem.at[t])
        own.start()
        owns.append(own)

    for off in range(1, n_sa):
        norm_sa_copies[off - 1].wait_recv()
        own_norm = own_norm + norm_sa_recv[off - 1]
    norm_ta_send[...] = own_norm
    for off in range(1, n_ta):
        copy = pltpu.make_async_remote_copy(
            src_ref=norm_ta_send,
            dst_ref=norm_ta_recv.at[off - 1],
            send_sem=ta_out_sems.at[off - 1],
            recv_sem=ta_in_sems.at[off - 1],
            device_id={"ta": lax.rem(my_ta + off, n_ta)},
        )
        copy.start()
        norm_ta_copies.append(copy)

    for t in range(slices):
        owns[t].wait()
        total = recv_buf[t, pl.ds((n_sa - 1) * rows, rows), :]
        for off in range(1, n_sa):
            copies[t, off].wait_recv()
            total = total + recv_buf[t, pl.ds((off - 1) * rows, rows), :]
        for p in range(parts):
            for r in range(rows_own):
                row = p * rows_own + r
                out_ref[p, pl.ds(t, 1), pl.ds(r * LANES, LANES)] = total[row : row + 1]
    for off in range(1, n_ta):
        norm_ta_copies[off - 1].wait_recv()
        own_norm = own_norm + norm_ta_recv[off - 1]
    cells = 1.0 * spins * colors * slices * n_ta * sites * n_sa
    own_norm = own_norm / cells
    for s in range(srcs):
        norm_ref[pl.ds(s, 1), :] = own_norm[:, s * cols : (s + 1) * cols]
    for copy in norm_sa_copies + norm_ta_copies:
        copy.wait_send()
    for copy in copies.values():
        copy.wait_send()


def hand_over(tiles_ref, norms_ref, out_ref, norm_ref):
    out_ref[...] = tiles_ref[...]
    norm_ref[...] = norms_ref[...]


def on_device(eigvecs, solutions, source_times, spin_dilution):
    n_ta, n_sa = lax.axis_size("ta"), lax.axis_size("sa")
    parts, slices, eigs, colors, sites = eigvecs.shape
    _, _, srcs, cols, spins, _, _ = solutions.shape
    columns = srcs * cols * spins
    width = eigs * columns // n_sa
    eig_view = jnp.transpose(eigvecs, (0, 1, 3, 2, 4))
    sol_view = jnp.transpose(solutions, (0, 1, 2, 3, 5, 4, 6)).reshape(
        parts, slices, srcs * cols, colors, spins, sites
    )
    dims = (n_ta, n_sa, parts, slices, eigs, colors, sites, srcs, cols, spins, width)
    blocks = sites // LANES
    inner = colors * sites
    rows = parts * (width // LANES)
    f32, bf16 = jnp.float32, jnp.bfloat16
    dma = pltpu.SemaphoreType.DMA
    tiles, norms = pl.pallas_call(
        functools.partial(kernel, dims),
        out_shape=(
            jax.ShapeDtypeStruct((parts, slices, width), f32),
            jax.ShapeDtypeStruct((srcs, cols), f32),
        ),
        in_specs=[
            pl.BlockSpec(memory_space=pltpu.HBM),
            pl.BlockSpec(memory_space=pltpu.HBM),
            pl.BlockSpec(memory_space=pltpu.HBM),
            pl.BlockSpec(memory_space=pltpu.HBM),
        ],
        out_specs=(
            pl.BlockSpec(memory_space=pltpu.VMEM),
            pl.BlockSpec(memory_space=pltpu.VMEM),
        ),
        scratch_shapes=[
            pltpu.VMEM((slices * colors, parts, eigs, sites), f32),
            pltpu.VMEM((slices * colors * blocks, parts, columns, LANES), f32),
            pltpu.VMEM((slices, 2 * parts * eigs, inner), bf16),
            pltpu.VMEM((slices, parts * LANES, inner), bf16),
            pltpu.VMEM((slices, parts * LANES, inner), bf16),
            pltpu.VMEM((slices, parts, eigs, LANES), f32),
            pltpu.VMEM((slices, parts, eigs * columns // LANES, LANES), f32),
            pltpu.VMEM((slices, n_sa * rows, LANES), f32),
            pltpu.VMEM((slices, n_sa * rows, LANES), f32),
            pltpu.VMEM((1, LANES), f32),
            pltpu.VMEM((n_sa - 1, 1, LANES), f32),
            pltpu.VMEM((1, LANES), f32),
            pltpu.VMEM((n_ta - 1, 1, LANES), f32),
            pltpu.SMEM((srcs,), jnp.int32),
            pltpu.SMEM((srcs, cols), jnp.int32),
            dma((2,)),
            dma((slices,)),
            dma((slices * colors,)),
            dma((slices * colors * blocks,)),
            dma((slices, n_sa - 1)),
            dma((slices, n_sa - 1)),
            dma((n_sa - 1,)),
            dma((n_sa - 1,)),
            dma((n_ta - 1,)),
            dma((n_ta - 1,)),
        ],
        compiler_params=pltpu.CompilerParams(collective_id=0, has_side_effects=True),
    )(eig_view, sol_view, source_times, spin_dilution)
    return pl.pallas_call(
        hand_over,
        out_shape=(
            jax.ShapeDtypeStruct(tiles.shape, f32),
            jax.ShapeDtypeStruct(norms.shape, f32),
        ),
    )(tiles, norms)


def solution(mesh):
    return jax.shard_map(
        on_device,
        mesh=mesh,
        in_specs=(
            P(None, "ta", None, None, "sa"),
            P(None, "ta", None, None, None, None, "sa"),
            P(),
            P(),
        ),
        out_specs=(P(None, "ta", "sa"), P()),
        check_vma=False,
    )
```

```python
import functools
import math

import jax
import jax.numpy as jnp
from jax import lax
from jax.experimental import pallas as pl
from jax.experimental.pallas import tpu as pltpu
from jax.sharding import PartitionSpec as P

LANES = 128
DIRECT = 64
NT_DIMS = (((1,), (1,)), ((), ()))


def split_two(x):
    high = x.astype(jnp.bfloat16)
    low = (x - high.astype(jnp.float32)).astype(jnp.bfloat16)
    return high, low


def kernel(
    dims,
    eig_hbm, sol_hbm, times_hbm, spin_hbm,
    out_ref, norm_ref,
    eig_buf, sol_buf, left, right_hi, right_lo, tile_buf, flat_buf,
    send_buf, recv_buf, norm_send, norm_recv,
    times_ref, spin_ref, small_sem, own_sem,
    eig_sem, sol_sem, out_sems, in_sems, norm_out_sems, norm_in_sems,
):
    n_ta, n_sa, parts, slices, eigs, colors, sites, srcs, cols, spins, width = dims
    columns = srcs * cols * spins
    rows_own = width // LANES
    blocks = sites // LANES
    my_ta, my_sa = lax.axis_index("ta"), lax.axis_index("sa")

    barrier = pltpu.get_barrier_semaphore()
    one_phase = n_ta * n_sa <= DIRECT
    every = [(a, b) for a in range(n_ta) for b in range(n_sa) if a or b]
    over_sa = [(0, b) for b in range(1, n_sa)]
    over_ta = [(a, 0) for a in range(1, n_ta)]
    first, second = (every, []) if one_phase else (over_sa, over_ta)

    def device(offs):
        return {
            "ta": lax.rem(my_ta + offs[0], n_ta),
            "sa": lax.rem(my_sa + offs[1], n_sa),
        }

    for offs in first + second:
        pl.semaphore_signal(barrier, inc=1, device_id=device(offs))

    small_copies = [
        pltpu.make_async_copy(times_hbm, times_ref, small_sem.at[0]),
        pltpu.make_async_copy(spin_hbm, spin_ref, small_sem.at[1]),
    ]
    for copy in small_copies:
        copy.start()
    sol_copies, eig_copies = {}, {}
    for t in range(slices):
        for c in range(colors):
            for j in range(blocks):
                at = (t * colors + c) * blocks + j
                copy = pltpu.make_async_copy(
                    sol_hbm.at[:, t, :, c, :, pl.ds(j * LANES, LANES)],
                    sol_buf.at[at].reshape(parts, srcs * cols, spins, LANES),
                    sol_sem.at[at],
                )
                copy.start()
                sol_copies[t, c, j] = copy
            copy = pltpu.make_async_copy(
                eig_hbm.at[:, t, c], eig_buf.at[t * colors + c], eig_sem.at[t * colors + c]
            )
            copy.start()
            eig_copies[t, c] = copy

    for copy in small_copies:
        copy.wait()
    lane = lax.broadcasted_iota(jnp.int32, (8, LANES), 1)
    chir = jnp.ones((8, LANES), jnp.float32)
    group = lane // spins
    for s in range(srcs):
        for k in range(cols):
            value = jnp.where(spin_ref[s, k] < 2, 1.0, -1.0)
            chir = jnp.where(group == s * cols + k, value, chir)
    source = lane // (spins * cols)
    signs = []
    for t in range(slices):
        now = my_ta * slices + t
        sign = chir
        for s in range(srcs):
            value = jnp.where(now < times_ref[s], -1.0, 1.0)
            sign = jnp.where(source == s, chir * value, sign)
        signs.append(sign[:1])

    period = math.lcm(columns, LANES)
    rows_in, rows_out = period // columns, period // LANES
    groups = eigs // rows_in
    lane_g = lax.broadcasted_iota(jnp.int32, (groups, LANES), 1)
    copies, owns = {}, []
    rows = parts * rows_own
    sub = math.gcd(rows, 4)

    def make_tiles(t):
        both = lax.dot_general(
            left[t], right_hi[t], NT_DIMS, preferred_element_type=jnp.float32
        )
        cross = lax.dot_general(
            left[t, : parts * eigs, :], right_lo[t], NT_DIMS,
            preferred_element_type=jnp.float32,
        )
        g = both[: parts * eigs] + both[parts * eigs :] + cross
        tiles = (
            g[:eigs, :LANES] + g[eigs:, LANES:],
            g[:eigs, LANES:] - g[eigs:, :LANES],
        )
        for p in range(parts):
            tile_buf[t, p] = tiles[p] * signs[t]
            taken = [tile_buf[t, p, pl.ds(i, groups, stride=rows_in), :] for i in range(rows_in)]
            for o in range(rows_out):
                value, filled = None, 0
                while filled < LANES:
                    i, skip = divmod(o * LANES + filled, columns)
                    size = min(columns - skip, LANES - filled)
                    shift = (filled - skip) % LANES
                    piece = pltpu.roll(taken[i], shift, 1) if shift else taken[i]
                    value = piece if value is None else jnp.where(lane_g < filled, value, piece)
                    filled += size
                flat_buf[t, p, pl.ds(o, groups, stride=rows_out), :] = value
            for d in range(n_sa):
                send_buf[t, pl.ds(d * rows + p * rows_own, rows_own), :] = flat_buf[
                    t, p, pl.ds(d * rows_own, rows_own), :
                ]

    def send_tiles(t):
        sent = send_buf.at[t].reshape(n_sa, rows // sub, sub, LANES)
        landed = recv_buf.at[t].reshape(n_sa, rows // sub, sub, LANES)
        for off in range(1, n_sa):
            peer = lax.rem(my_sa + off, n_sa)
            copy = pltpu.make_async_remote_copy(
                src_ref=sent.at[peer],
                dst_ref=landed.at[off - 1],
                send_sem=out_sems.at[t, off - 1],
                recv_sem=in_sems.at[t, off - 1],
                device_id={"sa": peer},
            )
            copy.start()
            copies[t, off] = copy
        own = pltpu.make_async_copy(sent.at[my_sa], landed.at[n_sa - 1], own_sem.at[t])
        own.start()
        owns.append(own)

    inner = colors * sites
    pad = LANES - columns
    if pad:
        for t in range(slices):
            for p in range(parts):
                spare = pl.ds(p * LANES + columns, pad)
                right_hi[t, spare, :] = jnp.zeros((pad, inner), jnp.bfloat16)
                right_lo[t, spare, :] = jnp.zeros((pad, inner), jnp.bfloat16)
    squares = jnp.zeros((columns, LANES), jnp.float32)
    for t in range(slices):
        for c in range(colors):
            for j in range(blocks):
                sol_copies[t, c, j].wait()
                lanes = pl.ds(c * sites + j * LANES, LANES)
                for p in range(parts):
                    x = sol_buf[(t * colors + c) * blocks + j, p]
                    squares = squares + x * x
                    high, low = split_two(x)
                    right_hi[t, pl.ds(p * LANES, columns), lanes] = high
                    right_lo[t, pl.ds(p * LANES, columns), lanes] = low
            eig_copies[t, c].wait()
            lanes = pl.ds(c * sites, sites)
            for p in range(parts):
                high, low = split_two(eig_buf[t * colors + c, p])
                left[t, pl.ds(p * eigs, eigs), lanes] = high
                left[t, pl.ds((parts + p) * eigs, eigs), lanes] = low
        if t < slices - 1:
            make_tiles(t)

    pl.semaphore_wait(barrier, len(first + second))

    precise = lax.Precision.HIGHEST
    lane_sums = lax.dot_general(
        jnp.ones((8, LANES), jnp.float32), squares, NT_DIMS,
        precision=precise, preferred_element_type=jnp.float32,
    )
    wanted = lax.broadcasted_iota(jnp.int32, (LANES, columns), 0)
    given = lax.broadcasted_iota(jnp.int32, (LANES, columns), 1) // spins
    picks = jnp.where(wanted == given, 1.0, 0.0).astype(jnp.float32)
    own_norm = lax.dot_general(
        lane_sums, picks, NT_DIMS, precision=precise, preferred_element_type=jnp.float32
    )[:1]
    norm_copies = []

    def send_norm(phase, base, peers):
        for at, offs in enumerate(peers):
            copy = pltpu.make_async_remote_copy(
                src_ref=norm_send.at[phase],
                dst_ref=norm_recv.at[base + at],
                send_sem=norm_out_sems.at[base + at],
                recv_sem=norm_in_sems.at[base + at],
                device_id=device(offs),
            )
            copy.start()
            norm_copies.append(copy)

    norm_send[0] = own_norm
    send_norm(0, 0, first)

    for t in range(slices):
        if t == slices - 1:
            make_tiles(t)
        send_tiles(t)

    if second:
        for at, copy in enumerate(norm_copies):
            copy.wait_recv()
            own_norm = own_norm + norm_recv[at]
        norm_send[1] = own_norm
        send_norm(1, len(first), second)

    for t in range(slices):
        owns[t].wait()
        total = recv_buf[t, pl.ds((n_sa - 1) * rows, rows), :]
        for off in range(1, n_sa):
            copies[t, off].wait_recv()
            total = total + recv_buf[t, pl.ds((off - 1) * rows, rows), :]
        for p in range(parts):
            for r in range(rows_own):
                row = p * rows_own + r
                out_ref[p, pl.ds(t, 1), pl.ds(r * LANES, LANES)] = total[row : row + 1]
    landed_from = len(first) if second else 0
    for copy in norm_copies[landed_from:]:
        copy.wait_recv()
    own_norm = own_norm + jnp.sum(norm_recv[landed_from:], axis=0)
    cells = 1.0 * spins * colors * slices * n_ta * sites * n_sa
    own_norm = own_norm / cells
    for s in range(srcs):
        norm_ref[pl.ds(s, 1), :] = own_norm[:, s * cols : (s + 1) * cols]
    for copy in norm_copies:
        copy.wait_send()
    for copy in copies.values():
        copy.wait_send()


def hand_over(tiles_ref, norms_ref, out_ref, norm_ref):
    out_ref[...] = tiles_ref[...]
    norm_ref[...] = norms_ref[...]


def on_device(eigvecs, solutions, source_times, spin_dilution):
    n_ta, n_sa = lax.axis_size("ta"), lax.axis_size("sa")
    parts, slices, eigs, colors, sites = eigvecs.shape
    _, _, srcs, cols, spins, _, _ = solutions.shape
    columns = srcs * cols * spins
    width = eigs * columns // n_sa
    eig_view = jnp.transpose(eigvecs, (0, 1, 3, 2, 4))
    sol_view = jnp.transpose(solutions, (0, 1, 2, 3, 5, 4, 6)).reshape(
        parts, slices, srcs * cols, colors, spins, sites
    )
    dims = (n_ta, n_sa, parts, slices, eigs, colors, sites, srcs, cols, spins, width)
    blocks = sites // LANES
    inner = colors * sites
    rows = parts * (width // LANES)
    norm_peers = n_ta * n_sa - 1 if n_ta * n_sa <= DIRECT else n_ta + n_sa - 2
    f32, bf16 = jnp.float32, jnp.bfloat16
    dma = pltpu.SemaphoreType.DMA
    tiles, norms = pl.pallas_call(
        functools.partial(kernel, dims),
        out_shape=(
            jax.ShapeDtypeStruct((parts, slices, width), f32),
            jax.ShapeDtypeStruct((srcs, cols), f32),
        ),
        in_specs=[
            pl.BlockSpec(memory_space=pltpu.HBM),
            pl.BlockSpec(memory_space=pltpu.HBM),
            pl.BlockSpec(memory_space=pltpu.HBM),
            pl.BlockSpec(memory_space=pltpu.HBM),
        ],
        out_specs=(
            pl.BlockSpec(memory_space=pltpu.VMEM),
            pl.BlockSpec(memory_space=pltpu.VMEM),
        ),
        scratch_shapes=[
            pltpu.VMEM((slices * colors, parts, eigs, sites), f32),
            pltpu.VMEM((slices * colors * blocks, parts, columns, LANES), f32),
            pltpu.VMEM((slices, 2 * parts * eigs, inner), bf16),
            pltpu.VMEM((slices, parts * LANES, inner), bf16),
            pltpu.VMEM((slices, parts * LANES, inner), bf16),
            pltpu.VMEM((slices, parts, eigs, LANES), f32),
            pltpu.VMEM((slices, parts, eigs * columns // LANES, LANES), f32),
            pltpu.VMEM((slices, n_sa * rows, LANES), f32),
            pltpu.VMEM((slices, n_sa * rows, LANES), f32),
            pltpu.VMEM((2, 1, LANES), f32),
            pltpu.VMEM((norm_peers, 1, LANES), f32),
            pltpu.SMEM((srcs,), jnp.int32),
            pltpu.SMEM((srcs, cols), jnp.int32),
            dma((2,)),
            dma((slices,)),
            dma((slices * colors,)),
            dma((slices * colors * blocks,)),
            dma((slices, n_sa - 1)),
            dma((slices, n_sa - 1)),
            dma((norm_peers,)),
            dma((norm_peers,)),
        ],
        compiler_params=pltpu.CompilerParams(collective_id=0, has_side_effects=True),
    )(eig_view, sol_view, source_times, spin_dilution)
    return pl.pallas_call(
        hand_over,
        out_shape=(
            jax.ShapeDtypeStruct(tiles.shape, f32),
            jax.ShapeDtypeStruct(norms.shape, f32),
        ),
    )(tiles, norms)


def solution(mesh):
    return jax.shard_map(
        on_device,
        mesh=mesh,
        in_specs=(
            P(None, "ta", None, None, "sa"),
            P(None, "ta", None, None, None, None, "sa"),
            P(),
            P(),
        ),
        out_specs=(P(None, "ta", "sa"), P()),
        check_vma=False,
    )
```
